32 devices in a mesh: dp: 2 (over x), tp: 16 (over y, z, core).
Axes of the slice: x: 2, y: 2, z: 4, core: 2. Of those that a mesh axis runs over, the one named last changes fastest.
Arguments:
- x: bfloat16 [4096, 7168], P('dp'), parts along dimension 0
- w_gate: bfloat16 [7168, 18432], P(None, 'tp')
- w_up: bfloat16 [7168, 18432], P(None, 'tp')
- w_down: bfloat16 [18432, 7168], P('tp')
Outputs:
- output: bfloat16 [4096, 7168], P('dp'), parts along dimension 0
There are 2 independent parts. The reference program is written for one: setup_inputs(seed, part) draws one part's arguments, and reference() takes and returns one part's arrays. A program takes and returns all parts, laid end to end along the dimension named above; an argument that names none is the same for every part.
All inputs are finite; a program needn't handle non-finite values.
Results may differ from the reference program's by a relative error of at most 0.016.
Values are sent between devices in bfloat16 or wider.
A program may use at most 2 GiB of HBM per device.

```python
import jax
import jax.numpy as jnp

ROWS = 2048
D = 7168
FF = 18432


def setup_inputs(seed: int = 0, part: int = 0) -> dict:
    kx, kg, ku, kd = jax.random.split(jax.random.key(seed), 4)
    drawn = {
        "x": jax.random.normal(jax.random.fold_in(kx, part), (ROWS, D), jnp.float32),
        "w_gate": jax.random.normal(kg, (D, FF), jnp.float32) * D**-0.5,
        "w_up": jax.random.normal(ku, (D, FF), jnp.float32) * D**-0.5,
        "w_down": jax.random.normal(kd, (FF, D), jnp.float32) * FF**-0.5,
    }
    return {k: v.astype(jnp.bfloat16) for k, v in drawn.items()}


def reference(x, w_gate, w_up, w_down):
    gate = jnp.dot(x, w_gate, preferred_element_type=jnp.float32)
    up = jnp.dot(x, w_up, preferred_element_type=jnp.float32)
    hidden = (jax.nn.silu(gate) * up).astype(jnp.bfloat16)
    return jnp.dot(hidden, w_down, preferred_element_type=jnp.float32).astype(jnp.bfloat16)
```

```python
import functools

import jax
import jax.numpy as jnp
from jax import lax
from jax.experimental import pallas as pl
from jax.experimental.pallas import tpu as pltpu
from jax.sharding import PartitionSpec as P

MESH = pl.DeviceIdType.MESH
F32, BF16 = jnp.float32, jnp.bfloat16

CH = 256
HALF = CH // 2
TN = 1024
KB = 1024
RAIL = 384
COMB = TN - RAIL
SLAB = 2 * RAIL + COMB
NB = 2
W = 4
WD = 8
WA = 8
LAST = 11
PARTS = 8


def kernel(x, wg, wu, wd, out, xb, wgu, wdb, acc, hid, part, psend, precv, gsend, grecv, ls, lra, lrb, xs, xr,
           sem_load, sem_wd, s_pair, r_pair, s_rung, r_rung, s_rs, r_a, r_b, s_x, r_x, s_c, r_c, s_r, r_r, s_g, r_g, s_d, r_d):
    rows, d = x.shape
    f = wg.shape[1]
    nt, nk, nch = d // TN, d // KB, rows // CH
    n = nt * nch
    div, rem = lax.div, lax.rem

    dp, tp = lax.axis_index("dp"), lax.axis_index("tp")
    y, z, c = div(tp, 8), rem(div(tp, 2), 4), rem(tp, 2)
    inner = jnp.logical_and(z >= 1, z <= 2)
    outer = jnp.logical_not(inner)
    low = z <= 1
    near = jnp.where(low, 0, 3)
    adj = jnp.where(low, 1, 2)
    opp = 3 - adj
    far = 3 - near

    def dev(yy, zz, cc):
        return (dp, (yy * 4 + zz) * 2 + cc)

    partner, rung = dev(y, z, 1 - c), dev(1 - y, z, c)
    to_adj, to_near, to_opp = dev(y, adj, c), dev(y, near, c), dev(y, opp, c)

    def remote(src, dst, ss, rs, to):
        return pltpu.make_async_remote_copy(src_ref=src, dst_ref=dst, send_sem=ss, recv_sem=rs, device_id=to, device_id_type=MESH)

    def loads(g):
        slot, b, j = rem(g, NB), rem(g, nk), div(g, nk)
        k0 = pl.ds(pl.multiple_of(b * KB, KB), KB)
        own = pl.ds(pl.multiple_of(j * CH + c * HALF, HALF), HALF)
        oth = pl.ds(pl.multiple_of(j * CH + (1 - c) * HALF, HALF), HALF)
        return (
            pltpu.make_async_copy(wg.at[k0, :], wgu.at[slot, :, pl.ds(0, f)], sem_load.at[slot, 0]),
            pltpu.make_async_copy(wu.at[k0, :], wgu.at[slot, :, pl.ds(f, f)], sem_load.at[slot, 1]),
            pltpu.make_async_copy(x.at[own, k0], xb.at[slot, pl.ds(0, HALF)], sem_load.at[slot, 2]),
            pltpu.make_async_copy(x.at[oth, k0], xb.at[slot, pl.ds(HALF, HALF)], sem_load.at[slot, 3]),
        )

    def load_wd(s):
        return pltpu.make_async_copy(wd.at[:, pl.ds(pl.multiple_of(rem(s, nt) * TN, TN), TN)], wdb.at[rem(s, 2)], sem_wd.at[rem(s, 2)])

    for g in range(NB):
        for cp in loads(jnp.int32(g)):
            cp.start()

    barrier = pltpu.get_barrier_semaphore()
    pl.semaphore_signal(barrier, 1, device_id=partner, device_id_type=MESH)
    pl.semaphore_signal(barrier, 1, device_id=rung, device_id_type=MESH)

    @pl.when(outer)
    def _():
        pl.semaphore_signal(barrier, 1, device_id=to_adj, device_id_type=MESH)
        pl.semaphore_wait(barrier, 3)

    @pl.when(inner)
    def _():
        pl.semaphore_signal(barrier, 1, device_id=to_near, device_id_type=MESH)
        pl.semaphore_signal(barrier, 1, device_id=to_opp, device_id_type=MESH)
        pl.semaphore_wait(barrier, 4)

    def gate_up(s, lo, hi):
        g = s + nk
        slot, b = rem(g, NB), rem(g, nk)

        @pl.when(g < nk * nch)
        def _():
            if lo == 0:
                for cp in loads(g):
                    cp.wait()
            for q in range(lo, hi):
                cs = slice(256 * q, 256 * (q + 1))
                r = jnp.dot(xb[slot], wgu[slot, :, cs], preferred_element_type=F32)
                acc[:, cs] = jnp.where(b == 0, 0.0, acc[:, cs]) + r
            if hi == 2 * f // 256:

                @pl.when(b == nk - 1)
                def _():
                    hs = rem(div(g, nk), 2)

                    def one(i, carry):
                        rs = pl.ds(pl.multiple_of(i * 16, 16), 16)
                        gate, up = acc[rs, :f], acc[rs, f:]
                        hid[hs, rs, :] = (jax.nn.silu(gate) * up).astype(BF16)
                        return carry

                    lax.fori_loop(0, CH // 16, one, 0)

                @pl.when(g + NB < nk * nch)
                def _():
                    for cp in loads(g + NB):
                        cp.start()

    def down(s, lo, hi):
        @pl.when(jnp.logical_and(s >= 0, s < n))
        def _():
            if lo == 0:
                load_wd(s).wait()
            hs = rem(div(s, nt), 2)
            for q in range(lo, hi):
                cs = slice(256 * q, 256 * (q + 1))
                r = jnp.dot(hid[hs], wdb[rem(s, 2), :, cs], preferred_element_type=F32)
                part[rem(s, WA), :, cs] = r[:HALF]
                psend[rem(s, 2), :, cs] = r[HALF:].astype(BF16)
            if hi == TN // 256:
                pair(s).start()

    def pair(p):
        return remote(psend.at[rem(p, 2)], precv.at[rem(p, W)], s_pair.at[rem(p, 2)], r_pair.at[rem(p, W)], partner)

    def rung_rs(p):
        return remote(gsend.at[rem(p, W)], grecv.at[rem(p, W)], s_rung.at[rem(p, W)], r_rung.at[rem(p, W)], rung)

    def rs(p, i, dst, sem, j, to):
        w = rem(p, W)
        return remote(ls.at[w, i], dst.at[w, j], s_rs.at[w, i], sem.at[w, j], to)

    def exch(p):
        w = rem(p, W)
        return remote(xs.at[w], xr.at[w], s_x.at[w], r_x.at[w], rung)

    def origin(p):
        return div(p, nt) * CH + c * HALF, rem(p, nt) * TN

    def comb_at(p, k):
        r0, c0 = origin(p)
        return out.at[pl.ds(pl.multiple_of(r0 + 64 * y + 16 * k, 16), 16), pl.ds(pl.multiple_of(c0 + RAIL, 128), COMB)]

    def rail_at(p, k):
        r0, c0 = origin(p)
        return out.at[pl.ds(pl.multiple_of(r0 + 32 * k, 32), 32), pl.ds(pl.multiple_of(c0, 128), RAIL)]

    def ag(at, ss, rs_, p, k, i, j, to):
        w = rem(p, W)
        return remote(at(p, k), at(p, k), ss.at[w, i], rs_.at[w, j], to)

    def rung_ag(p):
        r0, c0 = origin(p)
        ref = out.at[pl.ds(pl.multiple_of(r0 + 64 * y, 64), 64), pl.ds(pl.multiple_of(c0 + RAIL, 128), COMB)]
        return remote(ref, ref, s_g.at[rem(p, W)], r_g.at[rem(p, W)], rung)

    def core_ag(p):
        r0, c0 = origin(p)
        ref = out.at[pl.ds(pl.multiple_of(r0, HALF), HALF), pl.ds(pl.multiple_of(c0, 128), TN)]
        return remote(ref, ref, s_d.at[rem(p, WD)], r_d.at[rem(p, WD)], partner)

    def pieces(k):
        yield slice(0, RAIL), pl.ds(pl.multiple_of(32 * k, 16), 16), slice(0, RAIL)
        yield slice(RAIL, 2 * RAIL), pl.ds(pl.multiple_of(32 * k + 16, 16), 16), slice(0, RAIL)
        yield slice(2 * RAIL, SLAB), pl.ds(pl.multiple_of(64 * y + 16 * k, 16), 16), slice(RAIL, TN)

    def emit(p, k, i, src=None):
        w, a = rem(p, W), rem(p, WA)
        for cs, rw, cl in pieces(k):
            v = part[a, rw, cl]
            if src is not None:
                v = v + src[:, cs].astype(F32)
            ls[w, i, :, cs] = v.astype(BF16)

    def accumulate(p, k, src):
        a = rem(p, WA)
        for cs, rw, cl in pieces(k):
            part[a, rw, cl] = part[a, rw, cl] + src[:, cs].astype(F32)

    def root(p, src):
        w, a = rem(p, W), rem(p, WA)
        for i, (cs, rw, cl) in enumerate(pieces(z)):
            v = (part[a, rw, cl] + src[:, cs].astype(F32)).astype(BF16)
            if i < 2:
                xs[w, 16 * i : 16 * (i + 1), :] = v
            else:
                comb_at(p, z)[...] = v
        exch(p).start()

    def rail_final(p):
        w = rem(p, W)
        exch(p).wait()
        rail_at(p, z)[...] = (xs[w].astype(F32) + xr[w].astype(F32)).astype(BF16)

    def st1(p):
        pair(p).wait_recv()
        a, w = rem(p, WA), rem(p, W)
        for r in range(0, HALF, 16):
            rw = slice(r, r + 16)
            part[a, rw, :RAIL] = part[a, rw, :RAIL] + precv[w, rw, :RAIL].astype(F32)
        for r in range(0, 64, 16):
            mine = pl.ds(pl.multiple_of(64 * y + r, 16), 16)
            other = pl.ds(pl.multiple_of(64 * (1 - y) + r, 16), 16)
            gsend[w, r : r + 16, :] = (part[a, other, RAIL:] + precv[w, other, RAIL:].astype(F32)).astype(BF16)
            part[a, mine, RAIL:] = part[a, mine, RAIL:] + precv[w, mine, RAIL:].astype(F32)
        rung_rs(p).start()

    def st2(p):
        pair(p).wait_send()
        rung_rs(p).wait_recv()
        a, w = rem(p, WA), rem(p, W)
        for r in range(0, 64, 16):
            mine = pl.ds(pl.multiple_of(64 * y + r, 16), 16)
            part[a, mine, RAIL:] = part[a, mine, RAIL:] + grecv[w, r : r + 16, :].astype(F32)

        @pl.when(outer)
        def _():
            for i, k in ((2, far), (1, opp), (0, adj)):
                emit(p, k, i)
                rs(p, i, lra, r_a, i, to_adj).start()

    def st3(p):
        rung_rs(p).wait_send()
        w = rem(p, W)

        @pl.when(inner)
        def _():
            for j, k, i in ((2, far, 1), (1, opp, 0)):
                rs(p, j, lra, r_a, j, to_near).wait_recv()
                emit(p, k, i, lra.at[w, j])
                rs(p, i, lrb, r_b, i, to_opp).start()
            rs(p, 0, lra, r_a, 0, to_near).wait_recv()
            accumulate(p, z, lra.at[w, 0])

    def st4(p):
        w = rem(p, W)

        @pl.when(inner)
        def _():
            rs(p, 1, lrb, r_b, 1, to_opp).wait_recv()
            emit(p, near, 2, lrb.at[w, 1])
            rs(p, 2, lrb, r_b, 0, to_near).start()
            rs(p, 0, lrb, r_b, 0, to_opp).wait_recv()
            root(p, lrb.at[w, 0])
            ag(comb_at, s_c, r_c, p, z, 0, 0, to_near).start()
            ag(comb_at, s_c, r_c, p, z, 1, 0, to_opp).start()

        @pl.when(outer)
        def _():
            for i in range(3):
                rs(p, i, lra, r_a, i, to_adj).wait_send()

    def spread(at, ss, rr, p, q):
        def hop(k, i, j, to):
            return ag(at, ss, rr, p, k, i, j, to)

        if q == 1:

            @pl.when(outer)
            def _():
                hop(z, 0, 1, to_adj).start()
                hop(adj, 0, 0, to_adj).wait_recv()

            @pl.when(inner)
            def _():
                hop(opp, 0, 0, to_opp).wait_recv()
                hop(opp, 2, 1, to_near).start()

        if q == 2:

            @pl.when(inner)
            def _():
                hop(near, 0, 1, to_near).wait_recv()
                hop(near, 3, 2, to_opp).start()
                hop(z, 0, 0, to_near).wait_send()
                hop(z, 1, 0, to_opp).wait_send()

            @pl.when(outer)
            def _():
                hop(opp, 0, 1, to_adj).wait_recv()

        if q == 3:

            @pl.when(inner)
            def _():
                hop(far, 0, 2, to_opp).wait_recv()
                hop(far, 4, 2, to_near).start()
                hop(opp, 2, 1, to_near).wait_send()

            @pl.when(outer)
            def _():
                hop(z, 0, 1, to_adj).wait_send()

        if q == 4:

            @pl.when(outer)
            def _():
                hop(far, 0, 2, to_adj).wait_recv()

            @pl.when(inner)
            def _():
                hop(near, 3, 2, to_opp).wait_send()

        if q == 5:

            @pl.when(inner)
            def _():
                hop(far, 4, 2, to_near).wait_send()

    comb = functools.partial(spread, comb_at, s_c, r_c)
    rail = functools.partial(spread, rail_at, s_r, r_r)

    def st5(p):
        w = rem(p, W)

        @pl.when(outer)
        def _():
            rs(p, 0, lrb, r_b, 0, to_adj).wait_recv()
            root(p, lrb.at[w, 0])

        @pl.when(inner)
        def _():
            for i in range(2):
                rs(p, i, lrb, r_b, i, to_opp).wait_send()
            rail_final(p)
            ag(rail_at, s_r, r_r, p, z, 0, 0, to_near).start()
            ag(rail_at, s_r, r_r, p, z, 1, 0, to_opp).start()

        comb(p, 1)

    def st6(p):
        @pl.when(outer)
        def _():
            rail_final(p)

        @pl.when(inner)
        def _():
            rs(p, 2, lrb, r_b, 0, to_near).wait_send()

        comb(p, 2)
        rail(p, 1)

    def st7(p):
        comb(p, 3)
        rail(p, 2)

    def st8(p):
        comb(p, 4)
        rung_ag(p).start()
        rail(p, 3)

    def st9(p):
        comb(p, 5)
        rail(p, 4)
        rung_ag(p).wait_recv()
        core_ag(p).start()

    def st10(p):
        rail(p, 5)
        rung_ag(p).wait_send()

    def st11(p):
        core_ag(p).wait()

    stages = (None, st1, st2, st3, st4, st5, st6, st7, st8, st9, st10, st11)

    def run(s, qs):
        for q in qs:
            p = s - q

            @pl.when(jnp.logical_and(p >= 0, p < n))
            def _():
                stages[q](p)

    def body(i, carry):
        s = i - nk
        run(s, (1, 2))
        gate_up(s, 0, 3)
        run(s, (3, 4))
        gate_up(s, 3, 6)
        run(s, (5, 6))
        gate_up(s, 6, 9)
        run(s, (7, 8, 9))

        @pl.when(jnp.logical_and(s >= -1, s < n - 1))
        def _():
            load_wd(s + 1).start()

        down(s, 0, 2)
        run(s, (10, 11))
        down(s, 2, 4)
        return carry

    lax.fori_loop(0, nk + n + LAST, body, 0)


def flush(src, dst, sem):
    rows = src.shape[0] // PARTS
    cps = [pltpu.make_async_copy(src.at[pl.ds(i * rows, rows)], dst.at[pl.ds(i * rows, rows)], sem.at[i]) for i in range(PARTS)]
    for cp in cps:
        cp.start()
    for cp in cps:
        cp.wait()


def solution(mesh):
    def step(x, wg, wu, wd):
        rows, d = x.shape
        f = wg.shape[1]
        sem = pltpu.SemaphoreType.DMA
        any_ = pl.BlockSpec(memory_space=pl.ANY)
        whole = pl.pallas_call(
            kernel,
            out_shape=pltpu.VMEM((rows, d), BF16),
            in_specs=[any_] * 4,
            out_specs=pl.BlockSpec(memory_space=pltpu.VMEM),
            scratch_shapes=[
                pltpu.VMEM((NB, CH, KB), BF16),
                pltpu.VMEM((NB, KB, 2 * f), BF16),
                pltpu.VMEM((2, f, TN), BF16),
                pltpu.VMEM((CH, 2 * f), F32),
                pltpu.VMEM((2, CH, f), BF16),
                pltpu.VMEM((WA, HALF, TN), F32),
                pltpu.VMEM((2, HALF, TN), BF16),
                pltpu.VMEM((W, HALF, TN), BF16),
                pltpu.VMEM((W, 64, COMB), BF16),
                pltpu.VMEM((W, 64, COMB), BF16),
                pltpu.VMEM((W, 3, 16, SLAB), BF16),
                pltpu.VMEM((W, 3, 16, SLAB), BF16),
                pltpu.VMEM((W, 2, 16, SLAB), BF16),
                pltpu.VMEM((W, 32, RAIL), BF16),
                pltpu.VMEM((W, 32, RAIL), BF16),
                sem((NB, 4)),
                sem((2,)),
                sem((2,)),
                sem((W,)),
                sem((W,)),
                sem((W,)),
                sem((W, 3)),
                sem((W, 3)),
                sem((W, 2)),
                sem((W,)),
                sem((W,)),
                sem((W, 5)),
                sem((W, 3)),
                sem((W, 5)),
                sem((W, 3)),
                sem((W,)),
                sem((W,)),
                sem((WD,)),
                sem((WD,)),
            ],
            compiler_params=pltpu.CompilerParams(collective_id=0, has_side_effects=True, vmem_limit_bytes=33 * 2**20),
            cost_estimate=pl.CostEstimate(flops=6 * rows * d * f, bytes_accessed=400 * 2**20, transcendentals=rows * f),
        )(x, wg, wu, wd)
        return pl.pallas_call(
            flush,
            out_shape=jax.ShapeDtypeStruct((rows, d), BF16),
            in_specs=[pl.BlockSpec(memory_space=pltpu.VMEM)],
            out_specs=any_,
            scratch_shapes=[sem((PARTS,))],
            compiler_params=pltpu.CompilerParams(vmem_limit_bytes=2**20),
        )(whole)

    return jax.shard_map(
        step,
        mesh=mesh,
        in_specs=(P("dp", None), P(None, "tp"), P(None, "tp"), P("tp", None)),
        out_specs=P("dp", None),
        check_vma=False,
    )
```
